32 devices in a mesh: dp: 32 (over z, y, x, core), tensor: 1.
Axes of the slice: x: 2, y: 2, z: 4, core: 2. Of those that a mesh axis runs over, the one named last changes fastest.
Arguments:
- grad_codes: bfloat16 [4, 32, 32, 18432], P(None, 'dp', None, 'tensor'), may hold values from -448 to 448
- exponents: int32 [4, 32, 16], P(None, 'dp'), may hold values from 7 to 10
- accumulated: bfloat16 [32, 18432], P('dp', 'tensor'), may hold values from -12 to 12
- arrival: int32 [32], replicated, may hold values from 0 to 31, each once
- bucket_of_row: int32 [32], replicated, may hold values from 0 to 15, never falling along the last dimension, each value on 1 to 4 neighbouring positions
Outputs:
- unit_codes: bfloat16 [4, 32, 18432], P(None, 'dp', 'tensor')
- bucket_peaks: float32 [4, 16], replicated
- compensated: float32 [32, 18432], P('dp', 'tensor')
The draws below stay inside these ranges and needn't reach their ends.
Inputs may be any that keep to these rules, and one draw needn't show every extreme that they name: `arrival`: each weight row appears in exactly one slot. `bucket_of_row`: bucket numbers never fall along the rows; each bucket holds 1 to 4 consecutive rows and one holds exactly 4.
All inputs are finite; a program needn't handle non-finite values.
Results may differ from the reference program's by a relative error of at most 0.001.
Values sent between devices are 32-bit elements; how exact they have to be, the bound alone decides.
A program may use at most 64 MiB of HBM per device.

```python
import math
import jax
import jax.numpy as jnp
import numpy as np
from jax import lax

FF = 18432
STEPS = 4
NB = 16
ROWS = 32
REPLICAS = 32
BMOST = 4


def plant(array, rng, least, high):
    longest = array.shape.index(max(array.shape))
    spots = []
    for shift in (0, 1):
        where = [jax.random.randint(jax.random.fold_in(rng, axis), (), 0, length) for axis, length in enumerate(array.shape)]
        where[longest] = (where[longest] + shift) % array.shape[longest]
        spots.append(tuple(where))
    return array.at[spots[0]].set(least).at[spots[1]].set(high)


def raised(drawn, stream_key, source, target, blocks, factor):
    def block_of(axis_at):
        return (jnp.arange(drawn.shape[axis_at]) // (drawn.shape[axis_at] // blocks)).reshape((-1,) + (1,) * (drawn.ndim - 1 - axis_at))

    first = jax.random.permutation(stream_key, blocks)[block_of(target)]
    second = (block_of(target) + blocks // 2) % blocks
    return jnp.where((block_of(source) == first) | (block_of(source) == second), factor * drawn, drawn)


def levels(stream_key, extent, shards, low, high):
    def one(position, shards_of):
        draws = jax.random.uniform(jax.random.fold_in(jax.random.fold_in(stream_key, 6), position), (shards_of,), jnp.float32, low / len(shards), high / len(shards))
        return jnp.repeat(jnp.exp(draws), extent[position] // shards_of).reshape((-1,) + (1,) * (len(extent) - position - 1))

    factor_of = one(*shards[0])
    for cut in shards[1:]:
        factor_of = factor_of * one(*cut)
    return factor_of


def profile(amount, total, most, skew):
    loads = [(1 << 20) // math.isqrt(standing ** skew) + 1 for standing in range(2, amount + 1)]
    rest, counts = total - most - (amount - 1), [1] * (amount - 1)
    while rest > 0:
        free = [i for i in range(amount - 1) if counts[i] < most]
        whole, left = sum([loads[i] for i in free]), rest
        for i in free:
            extra = min(most - counts[i], max(1, left * loads[i] // whole), rest)
            counts[i] = counts[i] + extra
            rest = rest - extra
    return np.array([most] + counts)


def ragged(own_key, number_of, total, most, lean):
    if number_of == 2:
        one = jax.random.randint(own_key, (), max(1, total - most), min(most, total - 1) + 1)
        return jnp.stack([one, total - one])
    sizes = jnp.asarray(profile(number_of, total, most, lean), jnp.int32)
    twos = (number_of - 1) // 2
    source_of, receiver = sizes[1:1 + 2 * twos:2], sizes[2:2 + 2 * twos:2]
    room = jnp.minimum(source_of - 1, most - receiver)
    shifted = jax.random.randint(jax.random.fold_in(own_key, 1), (twos,), 0, 1 << 20) % (room + 1)
    sizes = sizes.at[1:1 + 2 * twos:2].set(source_of - shifted).at[2:2 + 2 * twos:2].set(receiver + shifted)
    return sizes[jax.random.permutation(jax.random.fold_in(own_key, 2), number_of)]


def gaussian(key, dims, deviation, most, split=(), kind=jnp.bfloat16):
    array = jax.random.normal(key, dims, jnp.float32) * deviation
    if len(split) > 0:
        array = levels(key, dims, split, -0.22, 0.18) * array
    return jnp.clip(array, min=-most, max=most).astype(kind)


def noise_with(key, extent, width, reach, pieces, heavy, held_as=jnp.bfloat16):
    drawn = width * jax.random.normal(key, extent, jnp.float32)
    if pieces:
        drawn = drawn * levels(key, extent, pieces, -0.22, 0.18)
    return jnp.clip(raised(drawn, jax.random.fold_in(key, 3), *heavy), -reach, reach).astype(held_as)


def setup_inputs(seed: int = 0) -> dict:
    key_list = jax.random.split(jax.random.key(seed), 6)
    grad_codes = noise_with(key_list[0], (STEPS, REPLICAS, ROWS, FF), 64.0, 448.0, ((1, 32),), (1, 2, 32, 2.75))
    exponents = plant(jax.random.randint(key_list[1], (STEPS, REPLICAS, NB), 7, 11), jax.random.fold_in(key_list[1], 1), 7, 10).astype(jnp.int32)
    accumulated = gaussian(key_list[2], (ROWS, FF), 2.0, 12.0, ((0, 32),))
    arrival = jax.random.permutation(key_list[3], ROWS).astype(jnp.int32)
    bucket_of_row = jnp.searchsorted(jnp.cumsum(ragged(key_list[4], NB, ROWS, BMOST, 1)), jnp.arange(ROWS), side="right").astype(jnp.int32)
    return {"grad_codes": grad_codes, "exponents": exponents, "accumulated": accumulated, "arrival": arrival, "bucket_of_row": bucket_of_row}


epsilon = 1e-6


def reference(grad_codes, exponents, accumulated, arrival, bucket_of_row):
    inverse = jnp.zeros((ROWS,), jnp.int32).at[arrival].set(jnp.arange(ROWS, dtype=jnp.int32))
    member = bucket_of_row[:, None] == jnp.arange(NB, dtype=jnp.int32)[None, :]

    def add_replica(running_sum, replica_item):
        row_block, exponent_row = replica_item
        factor = jnp.exp2(-exponent_row.astype(jnp.float32))
        factor_rows = jnp.sum(jnp.where(member, factor[None, :], jnp.float32(0.0)), axis=1)
        picked = jnp.take(row_block, inverse, axis=0).astype(jnp.float32)
        return running_sum + picked * factor_rows[:, None], None

    running = accumulated
    carried = jnp.zeros((ROWS, FF), jnp.float32)
    unit_list = []
    peak_list = []
    exact_sum = carried
    for micro_step in range(STEPS):
        reduced, _ = lax.scan(add_replica, jnp.zeros((ROWS, FF), jnp.float32),
                              (grad_codes[micro_step], exponents[micro_step]))
        adjusted = reduced - carried
        previous = running.astype(jnp.float32)
        running = lax.optimization_barrier((previous + adjusted).astype(jnp.bfloat16))
        carried = (running.astype(jnp.float32) - previous) - adjusted
        exact_sum = running.astype(jnp.float32) - carried
        row_max = jnp.max(jnp.abs(exact_sum), axis=1)
        peaks = jnp.max(jnp.where(member, row_max[:, None], jnp.float32(0.0)), axis=0)
        peak_rows = jnp.sum(jnp.where(member, peaks[None, :], jnp.float32(0.0)), axis=1)
        unit_list.append((exact_sum / (peak_rows[:, None] + epsilon)).astype(jnp.bfloat16))
        peak_list.append(peaks)
    return jnp.stack(unit_list), jnp.stack(peak_list), exact_sum
```

```python
import functools

import jax
import jax.numpy as jnp
from jax import lax
from jax.experimental import pallas as pl
from jax.experimental.pallas import tpu as pltpu
from jax.sharding import PartitionSpec as P

epsilon = 1e-06
LANES = 128


def bit_orders(bits):
    head = list(range(1, min(4, bits)))
    tail = list(range(1 + len(head), bits))
    return [[0] + head[r:] + head[:r] + tail for r in range(max(1, len(head)))]


def widths_of(tiles, count):
    if count == 1:
        return [tiles]
    first = -(-tiles * 8 // 18)
    last = tiles * 4 // 18
    return [first, tiles - first - last, last]


def exchange(n, steps, rows, groups, orders, spans, codes, meta, start, exact, table, x, lhs, out, acc, r0, r1, peak,
             x_sem, send_sem, recv_sem, peak_send, peak_recv):
    me = lax.axis_index("dp")
    bits = n.bit_length() - 1
    half = rows // 2
    width = x.shape[2]
    lands = [r0] + list(r1)
    loads = []
    for s in range(steps):
        for g in range(groups):
            copy = pltpu.make_async_copy(
                codes.at[s, 0, :, pl.ds(g * width, width)], x.at[s, pl.ds(g * rows, rows), :], x_sem.at[s, g]
            )
            copy.start()
            loads.append(copy)

    barrier = pltpu.get_barrier_semaphore()

    def greet(j, carry):
        pl.semaphore_signal(barrier, inc=1, device_id={"dp": lax.rem(me + j, n)}, device_id_type=pl.DeviceIdType.MESH)
        return carry

    lax.fori_loop(1, n, greet, 0)

    partners = []
    for b in range(bits):
        stride = 1 << b
        bit = lax.rem(me // stride, 2)
        partners.append(me + stride * (1 - 2 * bit))

    size = groups * rows
    row_id = lax.broadcasted_iota(jnp.int32, (size, size), 0)
    col_id = lax.broadcasted_iota(jnp.int32, (size, size), 1)
    same_group = (row_id % groups) == (col_id // rows)
    position = row_id // groups
    masks = []
    for order in orders:
        owner = jnp.zeros_like(position)
        for m, b in enumerate(order):
            bit = (position // (1 << (bits - 1 - m))) % 2
            mine = lax.rem(me // (1 << b), 2)
            owner = owner + ((bit + mine) % 2) * (1 << b)
        masks.append(same_group & (owner.astype(jnp.float32) == meta[steps : steps + 1, :]))
    for q in range(len(orders)):
        for s in range(steps):
            lhs[q, s] = jnp.where(masks[q], meta[s : s + 1, :], 0.0).astype(jnp.bfloat16)

    def copy_of(s, q, k):
        at, wide = spans[q]
        count = half >> k
        source = out.at[s, :, :, pl.ds(at, wide)] if k == 0 else acc.at[s, pl.ds(count, count), :, pl.ds(at, wide)]
        return pltpu.make_async_remote_copy(
            src_ref=source,
            dst_ref=lands[k].at[s, :, :, pl.ds(at, wide)],
            send_sem=send_sem.at[s, q, k],
            recv_sem=recv_sem.at[s, q, k],
            device_id={"dp": partners[orders[q][k]]},
            device_id_type=pl.DeviceIdType.MESH,
        )

    def stage(s, q, k):
        at, wide = spans[q]
        cols = pl.ds(at, wide)
        if k == 0:
            split = half * groups
            part = jnp.dot(lhs[q, s, split:, :], x[s, :, cols], preferred_element_type=jnp.float32)
            out[s, :, :, cols] = part.reshape(half, groups, wide)
            if s == 0 and q == 0:
                pl.semaphore_wait(barrier, n - 1)
            copy_of(s, q, 0).start()
            part = jnp.dot(lhs[q, s, :split, :], x[s, :, cols], preferred_element_type=jnp.float32)
            acc[s, :, :, cols] = part.reshape(half, groups, wide)
            return
        copy_of(s, q, k - 1).wait_recv()
        count = half >> k
        got = lands[k - 1]
        if k < bits:
            acc[s, count : 2 * count, :, cols] += got[s, count : 2 * count, :, cols]
            copy_of(s, q, k).start()
            acc[s, 0:count, :, cols] += got[s, 0:count, :, cols]
        else:
            acc[s, 0:1, :, cols] += got[s, 0:1, :, cols]

    state = [start[...], jnp.zeros_like(start)]
    peaks = []
    for wave in range(steps + bits):
        for k in range(bits + 1):
            s = wave - k
            if s < 0 or s >= steps:
                continue
            if k == 0:
                for copy in loads[s * groups : (s + 1) * groups]:
                    copy.wait()
            for q in range(len(orders)):
                stage(s, q, k)
            if k == bits:
                running, carried = state
                adjusted = acc[s, 0] - carried
                new = (running + adjusted).astype(jnp.bfloat16).astype(jnp.float32)
                carried = (new - running) - adjusted
                state = [new, carried]
                total = new - carried
                exact[s] = total
                peaks.append(jnp.max(jnp.max(jnp.abs(total), axis=0, keepdims=True), axis=1, keepdims=True))

    lane = lax.broadcasted_iota(jnp.int32, (1, LANES), 1)
    row = jnp.zeros((1, LANES), jnp.float32)
    for s in range(steps):
        row = jnp.where(lane == s, peaks[s], row)
    peak[...] = row

    def peak_copy(j):
        return pltpu.make_async_remote_copy(
            src_ref=peak,
            dst_ref=table.at[me],
            send_sem=peak_send.at[j],
            recv_sem=peak_recv.at[j],
            device_id={"dp": lax.rem(me + j, n)},
            device_id_type=pl.DeviceIdType.MESH,
        )

    def tell(j, carry):
        peak_copy(j).start()
        return carry

    def hear(j, carry):
        peak_copy(j).wait()
        return carry

    lax.fori_loop(1, n, tell, 0)
    table[me] = row
    for s in range(steps):
        for q in range(len(orders)):
            for k in range(bits):
                copy_of(s, q, k).wait_send()
    lax.fori_loop(1, n, hear, 0)


def on_device(n, tensor, grad_codes, exponents, accumulated, arrival, bucket_of_row):
    steps, _, rows, columns = grad_codes.shape
    buckets = exponents.shape[2]
    bits = n.bit_length() - 1
    groups = max(g for g in (1, 2, 4, 8) if columns % (g * LANES) == 0)
    width = columns // groups
    orders = bit_orders(bits)
    spans, at = [], 0
    for tiles in widths_of(width // LANES, len(orders)):
        spans.append((at, tiles * LANES))
        at += tiles * LANES

    member = bucket_of_row[:, None] == jnp.arange(buckets, dtype=jnp.int32)[None, :]
    factors = jnp.exp2(-exponents[:, 0, :].astype(jnp.float32))
    factor_rows = jnp.sum(jnp.where(member[None], factors[:, None, :], 0.0), axis=2)
    holds = arrival[:, None] == jnp.arange(rows, dtype=jnp.int32)[None, :]
    factor_slots = jnp.sum(jnp.where(holds[None], factor_rows[:, None, :], 0.0), axis=2)
    meta = jnp.tile(jnp.concatenate([factor_slots, arrival[None].astype(jnp.float32)]), (1, groups))

    half = rows // 2
    vmem = pl.BlockSpec(memory_space=pltpu.VMEM)
    exact, table = pl.pallas_call(
        functools.partial(_entry, n, steps, rows, groups, orders, spans, bits),
        out_shape=(
            jax.ShapeDtypeStruct((steps, groups, width), jnp.float32),
            jax.ShapeDtypeStruct((n, 1, LANES), jnp.float32),
        ),
        in_specs=[pl.BlockSpec(memory_space=pl.ANY), vmem, vmem],
        out_specs=(vmem, vmem),
        scratch_shapes=[
            pltpu.VMEM((steps, groups * rows, width), jnp.bfloat16),
            pltpu.VMEM((len(orders), steps, groups * rows, groups * rows), jnp.bfloat16),
            pltpu.VMEM((steps, half, groups, width), jnp.float32),
            pltpu.VMEM((steps, half, groups, width), jnp.float32),
        ]
        + [pltpu.VMEM((steps, half >> k, groups, width), jnp.float32) for k in range(bits)]
        + [
            pltpu.VMEM((1, LANES), jnp.float32),
            pltpu.SemaphoreType.DMA((steps, groups)),
            pltpu.SemaphoreType.DMA((steps, len(orders), bits)),
            pltpu.SemaphoreType.DMA((steps, len(orders), bits)),
            pltpu.SemaphoreType.DMA((n,)),
            pltpu.SemaphoreType.DMA((n,)),
        ],
        compiler_params=pltpu.CompilerParams(
            collective_id=0, has_side_effects=True, vmem_limit_bytes=56 * 1024 * 1024
        ),
    )(grad_codes, meta, accumulated.astype(jnp.float32).reshape(groups, width))

    row_peaks = table[:, 0, :steps]
    peak_table = jnp.max(jnp.where(member[:, None, :], row_peaks[:, :, None], 0.0), axis=0)
    if tensor > 1:
        peak_table = lax.pmax(peak_table, "tensor")
    own = lax.dynamic_slice_in_dim(member, lax.axis_index("dp"), 1, 0)
    own_peaks = jnp.sum(jnp.where(own, peak_table, 0.0), axis=1)
    unit = (exact / (own_peaks[:, None, None] + epsilon)).astype(jnp.bfloat16)
    return unit.reshape(steps, 1, columns), peak_table, exact[-1].reshape(1, columns)


def _entry(n, steps, rows, groups, orders, spans, bits, codes, meta, start, exact, table, x, lhs, out, acc, *rest):
    lands, others = rest[:bits], rest[bits:]
    exchange(n, steps, rows, groups, orders, spans, codes, meta, start, exact, table, x, lhs, out, acc,
             lands[0], lands[1:], *others)


def solution(mesh):
    return jax.shard_map(
        functools.partial(on_device, mesh.shape["dp"], mesh.shape["tensor"]),
        mesh=mesh,
        in_specs=(P(None, "dp", None, "tensor"), P(None, "dp", None), P("dp", "tensor"), P(), P()),
        out_specs=(P(None, "dp", "tensor"), P(), P("dp", "tensor")),
        check_vma=False,
    )
```

```python
import functools

import jax
import jax.numpy as jnp
from jax import lax
from jax.experimental import pallas as pl
from jax.experimental.pallas import tpu as pltpu
from jax.sharding import PartitionSpec as P

epsilon = 1e-06
LANES = 128


def bit_orders(bits):
    head = list(range(1, min(4, bits)))
    tail = list(range(1 + len(head), bits))
    return [[0] + head[r:] + head[:r] + tail for r in range(max(1, len(head)))]


def chunks_of(tiles, count):
    plans = {18: PLAN}
    plan = plans.get(tiles, [(1,) * count] * (tiles // count)) if count == 3 else [(tiles,) + (0,) * (count - 1)]
    plan = [list(row) for row in plan]
    plan[0][0] += tiles - sum(map(sum, plan))
    spans, at = [], 0
    for row in plan:
        spans.append([])
        for wide in row:
            spans[-1].append((at * LANES, wide * LANES))
            at += wide
    return spans


PLAN = [(2, 1, 1), (2, 2, 1), (2, 2, 1), (2, 1, 1)]


def exchange(n, orders, spans, codes, exponents, accumulated, arrival, bucket_of_row, exact, peak_table, own_peak, x, lhs,
             begin, out, acc, peak, table, x_sem, send_sem, recv_sem, peak_send, peak_recv, *lands):
    me = lax.axis_index("dp")
    bits = n.bit_length() - 1
    steps, size, width = x.shape
    rows = codes.shape[2]
    groups = size // rows
    half = rows // 2
    loads = []
    for c, row in enumerate(spans):
        first, wide = row[0][0], sum(w for _, w in row)
        loads.append([])
        for g in range(groups):
            copy = pltpu.make_async_copy(
                codes.at[:, 0, :, pl.ds(g * width + first, wide)],
                x.at[:, pl.ds(g * rows, rows), pl.ds(first, wide)],
                x_sem.at[c, g],
            )
            copy.start()
            loads[-1].append(copy)

    barrier = pltpu.get_barrier_semaphore()

    def greet(j, carry):
        pl.semaphore_signal(barrier, inc=1, device_id={"dp": lax.rem(me + j, n)}, device_id_type=pl.DeviceIdType.MESH)
        return carry

    lax.fori_loop(1, n, greet, 0)

    partners = []
    for b in range(bits):
        stride = 1 << b
        bit = lax.rem(me // stride, 2)
        partners.append(me + stride * (1 - 2 * bit))

    slot = lax.broadcasted_iota(jnp.int32, (1, size), 1) % rows
    held = jnp.zeros((1, size), jnp.int32)
    scale = [jnp.zeros((1, size), jnp.int32) for _ in range(steps)]
    for k in range(rows):
        row = arrival[k]
        bucket = bucket_of_row[row]
        here = slot == k
        held = jnp.where(here, row, held)
        for s in range(steps):
            scale[s] = jnp.where(here, exponents[s, 0, bucket], scale[s])
    scale = [jnp.exp2(-e.astype(jnp.float32)) for e in scale]

    row_group = lax.broadcasted_iota(jnp.int32, (size, 1), 0) % groups
    col_group = lax.broadcasted_iota(jnp.int32, (1, size), 1) // rows
    wanted = held * groups + col_group
    place = lax.broadcasted_iota(jnp.int32, (size, 1), 0) // groups
    for q, order in enumerate(orders):
        owner = jnp.zeros_like(place)
        for m, b in enumerate(order):
            bit = (place // (1 << (bits - 1 - m))) % 2
            mine = lax.rem(me // (1 << b), 2)
            owner = owner + ((bit + mine) % 2) * (1 << b)
        mask = owner * groups + row_group == wanted
        for s in range(steps):
            lhs[q, s] = jnp.where(mask, scale[s], 0.0).astype(jnp.bfloat16)
    for g in range(groups):
        begin[g : g + 1, :] = accumulated[:, g * width : (g + 1) * width].astype(jnp.float32)

    def copy_of(c, q, k):
        at, wide = spans[c][q]
        count = half >> k
        cols = pl.ds(at, wide)
        source = out.at[:, :, :, cols] if k == 0 else acc.at[:, pl.ds(count, count), :, cols]
        return pltpu.make_async_remote_copy(
            src_ref=source,
            dst_ref=lands[k].at[:, :, :, cols],
            send_sem=send_sem.at[c, q, k],
            recv_sem=recv_sem.at[c, q, k],
            device_id={"dp": partners[orders[q][k]]},
            device_id_type=pl.DeviceIdType.MESH,
        )

    def stage(c, q, k):
        at, wide = spans[c][q]
        cols = pl.ds(at, wide)
        if k == 0:
            split = half * groups
            for s in range(steps):
                part = jnp.dot(lhs[q, s], x[s, :, cols], preferred_element_type=jnp.float32)
                out[s, :, :, cols] = part[split:].reshape(half, groups, wide)
                acc[s, :, :, cols] = part[:split].reshape(half, groups, wide)
            if c == 0 and q == 0:
                pl.semaphore_wait(barrier, n - 1)
            copy_of(c, q, 0).start()
            return
        copy_of(c, q, k - 1).wait_recv()
        count = half >> k
        got = lands[k - 1]
        if k < bits:
            acc[:, count : 2 * count, :, cols] += got[:, count : 2 * count, :, cols]
            copy_of(c, q, k).start()
            acc[:, 0:count, :, cols] += got[:, 0:count, :, cols]
        else:
            acc[:, 0:1, :, cols] += got[:, 0:1, :, cols]

    tops = [jnp.zeros((groups, 1), jnp.float32) for _ in range(steps)]
    for wave in range(len(spans) + bits):
        for k in range(bits + 1):
            c = wave - k
            if c < 0 or c >= len(spans):
                continue
            streams = [q for q in range(len(orders)) if spans[c][q][1]]
            if k == 0:
                for copy in loads[c]:
                    copy.wait()
            for q in streams:
                stage(c, q, k)
            if k == bits:
                first, wide = spans[c][0][0], sum(w for _, w in spans[c])
                running = begin[:, first : first + wide]
                carried = jnp.zeros_like(running)
                for s in range(steps):
                    adjusted = acc[s, 0, :, first : first + wide] - carried
                    new = (running + adjusted).astype(jnp.bfloat16).astype(jnp.float32)
                    carried = (new - running) - adjusted
                    running = new
                    total = new - carried
                    tops[s] = jnp.maximum(tops[s], jnp.max(jnp.abs(total), axis=1, keepdims=True))
                    for g in range(groups):
                        exact[s : s + 1, g * width + first : g * width + first + wide] = total[g : g + 1, :]

    lane = lax.broadcasted_iota(jnp.int32, (1, LANES), 1)
    row = jnp.zeros((1, LANES), jnp.float32)
    for s in range(steps):
        row = jnp.where(lane == s, jnp.max(tops[s], axis=0, keepdims=True), row)
    peak[...] = row

    def peak_copy(j):
        return pltpu.make_async_remote_copy(
            src_ref=peak,
            dst_ref=table.at[me],
            send_sem=peak_send.at[j],
            recv_sem=peak_recv.at[j],
            device_id={"dp": lax.rem(me + j, n)},
            device_id_type=pl.DeviceIdType.MESH,
        )

    def tell(j, carry):
        peak_copy(j).start()
        return carry

    def hear(j, carry):
        peak_copy(j).wait()
        return carry

    lax.fori_loop(1, n, tell, 0)
    table[me] = row
    for c in range(len(spans)):
        for q in range(len(orders)):
            if spans[c][q][1]:
                for k in range(bits):
                    copy_of(c, q, k).wait_send()
    lax.fori_loop(1, n, hear, 0)

    buckets = exponents.shape[2]
    by_bucket = jnp.zeros((buckets, LANES), jnp.float32)
    own = jnp.zeros((1, LANES), jnp.float32)
    bucket_id = lax.broadcasted_iota(jnp.int32, (buckets, LANES), 0)
    lane_id = lax.broadcasted_iota(jnp.int32, (buckets, LANES), 1)
    my_bucket = bucket_of_row[me]
    for i in range(rows):
        bucket = bucket_of_row[i]
        by_bucket = jnp.maximum(by_bucket, jnp.where(bucket_id == bucket, table[i], 0.0))
    own = jnp.max(jnp.where(bucket_id == my_bucket, by_bucket, 0.0), axis=0, keepdims=True)
    for s in range(steps):
        turned = jnp.sum(jnp.where(bucket_id == lane_id, by_bucket[:, s : s + 1], 0.0), axis=0, keepdims=True)
        peak_table[s : s + 1, :] = turned[:, :buckets]
        own_peak[s : s + 1, :] = jnp.broadcast_to(own[:, s : s + 1], (1, LANES))


def on_device(n, tensor, grad_codes, exponents, accumulated, arrival, bucket_of_row):
    steps, _, rows, columns = grad_codes.shape
    buckets = exponents.shape[2]
    bits = n.bit_length() - 1
    groups = max(g for g in (1, 2, 4, 8) if columns % (g * LANES) == 0)
    width = columns // groups
    orders = bit_orders(bits)
    spans = chunks_of(width // LANES, len(orders))
    half = rows // 2
    vmem = pl.BlockSpec(memory_space=pltpu.VMEM)
    smem = pl.BlockSpec(memory_space=pltpu.SMEM)
    exact, peak_table, own_peaks = pl.pallas_call(
        functools.partial(exchange, n, orders, spans),
        out_shape=(
            jax.ShapeDtypeStruct((steps, columns), jnp.float32),
            jax.ShapeDtypeStruct((steps, buckets), jnp.float32),
            jax.ShapeDtypeStruct((steps, LANES), jnp.float32),
        ),
        in_specs=[pl.BlockSpec(memory_space=pl.ANY), smem, vmem, smem, smem],
        out_specs=(vmem, vmem, vmem),
        scratch_shapes=[
            pltpu.VMEM((steps, groups * rows, width), jnp.bfloat16),
            pltpu.VMEM((len(orders), steps, groups * rows, groups * rows), jnp.bfloat16),
            pltpu.VMEM((groups, width), jnp.float32),
            pltpu.VMEM((steps, half, groups, width), jnp.float32),
            pltpu.VMEM((steps, half, groups, width), jnp.float32),
            pltpu.VMEM((1, LANES), jnp.float32),
            pltpu.VMEM((n, 1, LANES), jnp.float32),
            pltpu.SemaphoreType.DMA((len(spans), groups)),
            pltpu.SemaphoreType.DMA((len(spans), len(orders), bits)),
            pltpu.SemaphoreType.DMA((len(spans), len(orders), bits)),
            pltpu.SemaphoreType.DMA((n,)),
            pltpu.SemaphoreType.DMA((n,)),
        ]
        + [pltpu.VMEM((steps, half >> k, groups, width), jnp.float32) for k in range(bits)],
        compiler_params=pltpu.CompilerParams(
            collective_id=0, has_side_effects=True, vmem_limit_bytes=56 * 1024 * 1024
        ),
    )(grad_codes, exponents, accumulated, arrival, bucket_of_row)

    own_peaks = own_peaks[:, :1]
    if tensor > 1:
        peak_table = lax.pmax(peak_table, "tensor")
        own = lax.dynamic_slice_in_dim(bucket_of_row, lax.axis_index("dp"), 1, 0)
        own_member = own[:, None] == jnp.arange(buckets, dtype=jnp.int32)[None, :]
        own_peaks = jnp.max(jnp.where(own_member, peak_table, 0.0), axis=1, keepdims=True)
    unit = (exact / (own_peaks + epsilon)).astype(jnp.bfloat16)
    return unit.reshape(steps, 1, columns), peak_table, exact[steps - 1 :]


def solution(mesh):
    return jax.shard_map(
        functools.partial(on_device, mesh.shape["dp"], mesh.shape["tensor"]),
        mesh=mesh,
        in_specs=(P(None, "dp", None, "tensor"), P(None, "dp", None), P("dp", "tensor"), P(), P()),
        out_specs=(P(None, "dp", "tensor"), P(), P("dp", "tensor")),
        check_vma=False,
    )
```
